32 devices in a mesh: ep: 8 (over z, x), tp: 4 (over y, core).
Axes of the slice: x: 2, y: 2, z: 4, core: 2. Of those that a mesh axis runs over, the one named last changes fastest.
Arguments:
- hidden: bfloat16 [512, 2880], P('ep'), may hold values from -0.59765625 to 0.59765625
- queries: bfloat16 [512, 2048], P('ep', 'tp'), may hold values from -160 to 160
- new_keys: bfloat16 [512, 256], P('ep', 'tp'), may hold values from -6 to 6
- new_values: bfloat16 [512, 256], P('ep', 'tp'), may hold values from -6 to 6
- key_cache: bfloat16 [64, 4, 64, 1024], P('ep', 'tp'), may hold values from -6 to 6
- value_cache: bfloat16 [64, 4, 64, 1024], P('ep', 'tp'), may hold values from -6 to 6
- cache_lengths: int32 [64], P('ep'), may hold values from 16 to 1024
- w_out: bfloat16 [2048, 2880], P('tp'), may hold values from -0.125 to 0.125
- w_router: bfloat16 [2880, 8], replicated, may hold values from -0.109375 to 0.109375
- routes: int32 [512, 4], P('ep'), may hold values from 0 to 7, all different within a row; in each aligned block of 16 rows (0 to 15, 16 to 31, ...) at most 16 rows name the same one
- w_gate: bfloat16 [8, 2880, 1536], P('ep', None, 'tp'), may hold values from -0.109375 to 0.109375
- w_up: bfloat16 [8, 2880, 1536], P('ep', None, 'tp'), may hold values from -0.109375 to 0.109375
- w_down: bfloat16 [8, 1536, 2880], P('ep', 'tp'), may hold values from -0.15625 to 0.15625
Outputs:
- layer_out: bfloat16 [512, 2880], P(('ep', 'tp'))
The draws below stay inside these ranges and needn't reach their ends.
Inputs may be any that keep to these rules, and one draw needn't show every extreme that they name: `routes`: each token names 4 different experts; in each aligned block of 16 tokens no expert is named by more than 16 tokens, and in some blocks one expert is named by exactly 16.
All inputs are finite; a program needn't handle non-finite values.
Results may differ from the reference program's by a relative error of at most 0.02.
Values may be sent and summed in bfloat16 or wider, within the bound.
A program may use at most 64 MiB of HBM per device.

```python
import math
import jax
import jax.numpy as jnp
import numpy as np
from jax import lax

D = 2880
HEADS = 32
KV_HEADS = 4
HEAD_DIM = 64
FF = 1536
TOP = 4
SEQ_DEV = 8
LEN = 1024
EXPERTS = 8
SEQS = 64
TOKENS = 512
TOK_EP = 64
BLOCK = 16
CAP = 16
N_EP = 8
N_TP = 4


def draw_queries(key, part):
    shape_q = (TOKENS, HEADS * HEAD_DIM)
    values = jnp.clip(jax.random.normal(jax.random.fold_in(key, 1), shape_q, jnp.float32), -6.0, 6.0)
    return values.astype(jnp.bfloat16)


def draw_key_cache(key, part):
    base_draw = jax.random.normal(jax.random.fold_in(key, 3), (SEQS, KV_HEADS, HEAD_DIM, LEN), jnp.float32)
    base_draw = jnp.clip(base_draw, -6.0, 6.0)
    return base_draw.astype(jnp.bfloat16)


def place_ends(array, stream_key, low, high):
    dims = array.shape
    index_at = [jax.random.randint(jax.random.fold_in(stream_key, axis), (), 0, dims[axis]) for axis in range(len(dims))]
    array = array.at[tuple(index_at)].set(low)
    longest = dims.index(max(dims))
    index_at[longest] = (index_at[longest] + 1) % dims[longest]
    return array.at[tuple(index_at)].set(high)


def levels(key, dims, cuts, low, largest):
    gain = 1.0
    for axis_at, parts in cuts:
        steps = jax.random.uniform(jax.random.fold_in(jax.random.fold_in(key, 6), axis_at), (parts,), jnp.float32, low / len(cuts), largest / len(cuts))
        gain = gain * jnp.repeat(jnp.exp(steps), dims[axis_at] // parts).reshape((-1,) + (1,) * (len(dims) - 1 - axis_at))
    return gain


def deal_out(stream_key, own, number, rows, amount, top, reach, lean):
    ranking = jax.random.permutation(stream_key, amount)
    packed, common = portions_of(amount, rows * top, reach, lean, True), portions_of(amount, rows * top, reach, lean, False)
    places = jnp.arange(amount)

    def named(lengths, turn):
        used = int((lengths > 0).sum())
        fixed = max(1, used // 4)
        passed = fixed + (places - fixed + turn * (used - fixed)) % max(1, amount - fixed)
        return jnp.zeros((amount,), jnp.int32).at[ranking[jnp.where(places < fixed, places, passed)]].set(jnp.asarray(lengths, jnp.int32))

    lengths = jnp.where(number % 4 == 0, named(packed, number // 4), named(common, number - number // 4 - 1))
    mixed = jax.random.permutation(jax.random.fold_in(own, 3), amount)
    giver, receiver = mixed[0:amount // 2 * 2:2], mixed[1:amount // 2 * 2:2]
    slack = jnp.minimum(lengths[giver] - 1, reach - lengths[receiver]) // 2
    slack = jnp.where((giver == ranking[0]) | (receiver == ranking[0]) | (lengths[receiver] == 0), 0, jnp.maximum(slack, 0))
    passed = jax.random.randint(jax.random.fold_in(own, 4), (amount // 2,), 0, 1 << 20) % (slack + 1)
    lengths = lengths.at[giver].add(-passed).at[receiver].add(passed)
    items = jnp.searchsorted(jnp.cumsum(lengths), jnp.arange(rows * top), side="right").astype(jnp.int32)
    table = items.reshape(top, rows).T
    table = table[jax.random.permutation(jax.random.fold_in(own, 1), rows)]
    turn = jax.random.randint(jax.random.fold_in(own, 2), (rows, 1), 0, top)
    return jnp.take_along_axis(table, (jnp.arange(top)[None, :] + turn) % top, axis=1)


def portions_of(count, total, most, slope, full):
    weights = [(1 << 20) // math.isqrt(standing ** slope) + 1 for standing in range(1, count + 1)]
    largest = most if full else min(most, max(-(-total // count), total * weights[0] // sum(weights)))
    least = 1 if total - largest >= count - 1 else 0
    holding, rest = [largest] + [least] * (count - 1), total - largest - least * (count - 1)
    while rest > 0:
        movable = [i for i in range(1, count) if holding[i] < largest] or [i for i in range(1, count) if holding[i] < most]
        mass, left = sum([weights[i] for i in movable]), rest
        for i in movable:
            extra = min(most - holding[i], max(1, left * weights[i] // mass), rest)
            holding[i] = holding[i] + extra
            rest = rest - extra
    return np.array(holding)


def centred(key, dims, width, limit, split=(), kind=jnp.bfloat16):
    values = jax.random.normal(key, dims, jnp.float32) * width
    if len(split) > 0:
        values = levels(key, dims, split, -0.22, 0.18) * values
    return jnp.clip(values, min=-limit, max=limit).astype(kind)


def setup_inputs(seed: int = 0) -> dict:
    keys = jax.random.split(jax.random.key(seed), 14)
    hidden = centred(keys[0], (TOKENS, D), 0.1, 0.59765625, ((0, 8),))
    queries = draw_queries(jax.random.fold_in(keys[13], 71), 0)
    new_keys = centred(keys[2], (TOKENS, KV_HEADS * HEAD_DIM), 1.0, 6.0, ((0, 8), (1, 4)))
    new_values = centred(keys[3], (TOKENS, KV_HEADS * HEAD_DIM), 1.0, 6.0, ((0, 8), (1, 4)))
    key_cache = draw_key_cache(jax.random.fold_in(keys[13], 71), 0)
    value_cache = centred(keys[5], (SEQS, KV_HEADS, HEAD_DIM, LEN), 1.0, 6.0, ((0, 8), (1, 4)))
    cache_lengths = place_ends(jax.random.randint(keys[6], (SEQS,), 16, LEN + 1), jax.random.fold_in(keys[6], 1), 16, LEN).astype(jnp.int32)
    w_out = centred(keys[7], (HEADS * HEAD_DIM, D), (HEADS * HEAD_DIM) ** -0.5, 0.125, ((0, 4),))
    w_router = centred(keys[8], (D, EXPERTS), D ** -0.5, 0.109375)
    routes_keys = jax.random.split(jax.random.fold_in(keys[9], 1), TOKENS // BLOCK)
    routes_turns = jax.random.permutation(jax.random.fold_in(keys[9], 3), TOKENS // BLOCK)
    routes = jax.vmap(lambda own, number: deal_out(jax.random.fold_in(keys[9], 2), own, number, BLOCK, EXPERTS, TOP, CAP, 2))(routes_keys, routes_turns).reshape((TOKENS, TOP))
    w_gate = centred(keys[10], (EXPERTS, D, FF), D ** -0.5, 0.109375, ((0, 8), (2, 4)))
    w_up = centred(keys[11], (EXPERTS, D, FF), D ** -0.5, 0.109375, ((0, 8), (2, 4)))
    w_down = centred(keys[12], (EXPERTS, FF, D), FF ** -0.5, 0.15625, ((0, 8), (1, 4)))
    return dict(hidden=hidden, queries=queries, new_keys=new_keys, new_values=new_values, key_cache=key_cache, value_cache=value_cache, cache_lengths=cache_lengths, w_out=w_out, w_router=w_router, routes=routes, w_gate=w_gate, w_up=w_up, w_down=w_down)


def attend_block(queries, new_keys, new_values, key_cache, value_cache, cache_lengths):
    seq_count, kv_count, head_dim, length = key_cache.shape
    new_count = queries.shape[0] // seq_count
    group_size = queries.shape[1] // (kv_count * head_dim)
    row_count = new_count * group_size
    scale = head_dim ** (-0.5)
    query_block = queries.astype(jnp.float32).reshape(seq_count, new_count, kv_count, group_size, head_dim)
    query_block = query_block.transpose(0, 2, 1, 3, 4).reshape(seq_count, kv_count, row_count, head_dim)
    fresh_keys = new_keys.astype(jnp.float32).reshape(seq_count, new_count, kv_count, head_dim).transpose(0, 2, 1, 3)
    fresh_values = new_values.astype(jnp.float32).reshape(seq_count, new_count, kv_count, head_dim).transpose(0, 2, 1, 3)
    cache_scores = jnp.einsum('skrd,skdl->skrl', query_block, key_cache.astype(jnp.float32)) * scale
    in_cache = jnp.arange(length)[None, :] < cache_lengths[:, None]
    cache_scores = jnp.where(in_cache[:, None, None, :], cache_scores, -1e+30)
    fresh_scores = jnp.einsum('skrd,sknd->skrn', query_block, fresh_keys) * scale
    causal = (jnp.arange(row_count) // group_size)[:, None] >= jnp.arange(new_count)[None, :]
    fresh_scores = jnp.where(causal[None, None, :, :], fresh_scores, -1e+30)
    row_max = jnp.maximum(lax.optimization_barrier(jnp.max(cache_scores, -1, keepdims=True)), lax.optimization_barrier(jnp.max(fresh_scores, -1, keepdims=True)))
    cache_exp = jnp.exp(cache_scores - row_max)
    fresh_exp = jnp.exp(fresh_scores - row_max)
    denom_sum = lax.optimization_barrier(jnp.sum(cache_exp, -1, keepdims=True)) + lax.optimization_barrier(jnp.sum(fresh_exp, -1, keepdims=True))
    cache_probs = (cache_exp / denom_sum).astype(jnp.bfloat16).astype(jnp.float32)
    fresh_probs = (fresh_exp / denom_sum).astype(jnp.bfloat16).astype(jnp.float32)
    head_mix = jnp.einsum('skrl,skdl->skrd', cache_probs, value_cache.astype(jnp.float32))
    head_mix = head_mix + jnp.einsum('skrn,sknd->skrd', fresh_probs, fresh_values)
    head_mix = head_mix.reshape(seq_count, kv_count, new_count, group_size, head_dim).transpose(0, 2, 1, 3, 4)
    return head_mix.reshape(seq_count * new_count, kv_count * group_size * head_dim).astype(jnp.bfloat16)

def expert_rows(pieces):
    buffer_rows, gate_weight, up_weight, down_weight = pieces
    gate_proj = jnp.dot(buffer_rows, gate_weight, preferred_element_type=jnp.float32)
    up_proj = jnp.dot(buffer_rows, up_weight, preferred_element_type=jnp.float32)
    activated = ((up_proj + 1.0) * gate_proj * jax.nn.sigmoid(1.702 * gate_proj)).astype(jnp.bfloat16)
    return jnp.dot(activated, down_weight, preferred_element_type=jnp.float32)

def reference(hidden, queries, new_keys, new_values, key_cache, value_cache, cache_lengths, w_out, w_router, routes, w_gate, w_up, w_down):
    blocks = (queries.reshape(N_EP, TOK_EP, HEADS * HEAD_DIM), new_keys.reshape(N_EP, TOK_EP, KV_HEADS * HEAD_DIM), new_values.reshape(N_EP, TOK_EP, KV_HEADS * HEAD_DIM), key_cache.reshape(N_EP, SEQ_DEV, KV_HEADS, HEAD_DIM, LEN), value_cache.reshape(N_EP, SEQ_DEV, KV_HEADS, HEAD_DIM, LEN), cache_lengths.reshape(N_EP, SEQ_DEV))
    attended = lax.map(lambda pieces: attend_block(*pieces), blocks).reshape(TOKENS, HEADS * HEAD_DIM)
    residual = hidden.astype(jnp.float32) + jnp.dot(attended, w_out, preferred_element_type=jnp.float32)
    normed = (residual * lax.rsqrt(lax.optimization_barrier(jnp.mean(residual * residual, -1, keepdims=True)) + 1e-05)).astype(jnp.bfloat16)
    logits = jnp.dot(normed, w_router, preferred_element_type=jnp.float32)
    picked = jnp.take_along_axis(logits, routes, 1)
    picked_exp = jnp.exp(picked)
    weights = picked_exp / lax.optimization_barrier(jnp.sum(picked_exp, -1, keepdims=True))
    flat_routes = routes.reshape(-1).astype(jnp.int32)
    one_hot = (flat_routes[:, None] == jnp.arange(EXPERTS, dtype=jnp.int32)[None, :]).astype(jnp.int32)
    slot_rank = lax.optimization_barrier(jnp.sum((jnp.cumsum(one_hot, 0) - one_hot) * one_hot, 1)).astype(jnp.int32)
    capacity = N_EP * N_TP * CAP
    buffer = jnp.zeros((EXPERTS, capacity, D), jnp.bfloat16)
    buffer = buffer.at[flat_routes, slot_rank].set(jnp.repeat(normed, TOP, axis=0))
    outputs = lax.map(expert_rows, (buffer, w_gate, w_up, w_down))
    routed = outputs[flat_routes, slot_rank].reshape(TOKENS, TOP, D)
    mixture = lax.optimization_barrier(jnp.sum(weights[:, :, None] * routed, 1))
    return (residual + mixture).astype(jnp.bfloat16)
```

```python
import jax
import jax.numpy as jnp
from jax import lax
from jax.sharding import PartitionSpec as P


def attend(queries, new_keys, new_values, key_cache, value_cache, cache_lengths):
    seq_count, kv_count, head_dim, length = key_cache.shape
    new_count = queries.shape[0] // seq_count
    group_size = queries.shape[1] // (kv_count * head_dim)
    row_count = new_count * group_size
    scale = head_dim ** (-0.5)
    query_block = queries.reshape(seq_count, new_count, kv_count, group_size, head_dim)
    query_block = query_block.transpose(0, 2, 1, 3, 4).reshape(
        seq_count, kv_count, row_count, head_dim
    )
    fresh_keys = new_keys.reshape(seq_count, new_count, kv_count, head_dim).transpose(0, 2, 1, 3)
    fresh_values = new_values.reshape(seq_count, new_count, kv_count, head_dim).transpose(
        0, 2, 1, 3
    )
    cache_scores = (
        jnp.einsum("skrd,skdl->skrl", query_block, key_cache, preferred_element_type=jnp.float32)
        * scale
    )
    in_cache = jnp.arange(length)[None, :] < cache_lengths[:, None]
    cache_scores = jnp.where(in_cache[:, None, None, :], cache_scores, -1e30)
    fresh_scores = (
        jnp.einsum("skrd,sknd->skrn", query_block, fresh_keys, preferred_element_type=jnp.float32)
        * scale
    )
    causal = (jnp.arange(row_count) // group_size)[:, None] >= jnp.arange(new_count)[None, :]
    fresh_scores = jnp.where(causal[None, None, :, :], fresh_scores, -1e30)
    row_max = jnp.maximum(
        jnp.max(cache_scores, -1, keepdims=True), jnp.max(fresh_scores, -1, keepdims=True)
    )
    cache_exp = jnp.exp(cache_scores - row_max)
    fresh_exp = jnp.exp(fresh_scores - row_max)
    denom_sum = jnp.sum(cache_exp, -1, keepdims=True) + jnp.sum(fresh_exp, -1, keepdims=True)
    cache_probs = (cache_exp / denom_sum).astype(jnp.bfloat16)
    fresh_probs = (fresh_exp / denom_sum).astype(jnp.bfloat16)
    head_mix = jnp.einsum(
        "skrl,skdl->skrd", cache_probs, value_cache, preferred_element_type=jnp.float32
    )
    head_mix = head_mix + jnp.einsum(
        "skrn,sknd->skrd", fresh_probs, fresh_values, preferred_element_type=jnp.float32
    )
    head_mix = head_mix.reshape(seq_count, kv_count, new_count, group_size, head_dim).transpose(
        0, 2, 1, 3, 4
    )
    return head_mix.reshape(seq_count * new_count, kv_count * group_size * head_dim).astype(
        jnp.bfloat16
    )


def expert_apply(received, w_gate, w_up, w_down):
    width = received.shape[-1]
    flat_rows = received.reshape(-1, width)
    gate_proj = jnp.dot(flat_rows, w_gate[0], preferred_element_type=jnp.float32)
    up_proj = jnp.dot(flat_rows, w_up[0], preferred_element_type=jnp.float32)
    activated = ((up_proj + 1.0) * gate_proj * jax.nn.sigmoid(1.702 * gate_proj)).astype(
        jnp.bfloat16
    )
    partial_out = jnp.dot(activated, w_down[0], preferred_element_type=jnp.float32)
    return partial_out.reshape(received.shape[0], received.shape[1], width)


def dense_mix(residual, normed, weights, matches, w_gate, w_up, w_down):
    width = normed.shape[1]
    experts = matches.shape[2]
    dense = jnp.sum(jnp.where(matches, weights[:, :, None], 0.0), 1)
    high = dense.astype(jnp.bfloat16)
    low = (dense - high.astype(jnp.float32)).astype(jnp.bfloat16)
    rows = lax.all_gather(
        jnp.concatenate([normed, high, low], 1), ("ep", "tp"), axis=0, tiled=True
    )
    tokens = rows[:, :width]
    shares = rows[:, width : width + experts].astype(jnp.float32) + rows[
        :, width + experts :
    ].astype(jnp.float32)
    mine = jnp.arange(experts) == lax.axis_index("ep")
    share = jnp.sum(jnp.where(mine[None, :], shares, 0.0), 1, keepdims=True)
    partial_out = expert_apply(tokens[None], w_gate, w_up, w_down)[0]
    mixture = lax.psum_scatter(
        (share * partial_out).astype(jnp.bfloat16), ("ep", "tp"), scatter_dimension=0, tiled=True
    )
    return (residual + mixture.astype(jnp.float32)).astype(jnp.bfloat16)


def body(
    hidden,
    queries,
    new_keys,
    new_values,
    key_cache,
    value_cache,
    cache_lengths,
    w_out,
    w_router,
    routes,
    w_gate,
    w_up,
    w_down,
):
    tp_size = lax.axis_size("tp")
    tp_index = lax.axis_index("tp")
    width = hidden.shape[1]
    block_rows = hidden.shape[0] // tp_size
    top_count = routes.shape[1]
    experts = w_router.shape[1]
    capacity = min(block_rows, max(2, (2 * block_rows * top_count + experts - 1) // experts))
    start_row = tp_index * block_rows
    attended = attend(queries, new_keys, new_values, key_cache, value_cache, cache_lengths)
    partial_value = jnp.dot(attended, w_out, preferred_element_type=jnp.float32)
    summed = lax.psum_scatter(
        partial_value.astype(jnp.bfloat16), "tp", scatter_dimension=0, tiled=True
    ).astype(jnp.float32)
    residual = (
        lax.dynamic_slice_in_dim(hidden, start_row, block_rows, 0).astype(jnp.float32) + summed
    )
    local_routes = lax.dynamic_slice_in_dim(routes, start_row, block_rows, 0)
    block_count = 1
    normed = (
        residual * lax.rsqrt(jnp.mean(residual * residual, -1, keepdims=True) + 1e-05)
    ).astype(jnp.bfloat16)
    logits = jnp.dot(normed, w_router, preferred_element_type=jnp.float32)
    expert_ids = jnp.arange(experts, dtype=jnp.int32)
    matches = local_routes[:, :, None] == expert_ids[None, None, :]
    picked = jnp.sum(jnp.where(matches, logits[:, None, :], 0.0), -1)
    picked_exp = jnp.exp(picked)
    weights = picked_exp / jnp.sum(picked_exp, -1, keepdims=True)
    if capacity >= block_rows:
        return dense_mix(residual, normed, weights, matches, w_gate, w_up, w_down)
    flat_routes = local_routes.reshape(-1)
    one_hot = (
        flat_routes.reshape(block_count, block_rows * top_count)[:, :, None]
        == expert_ids[None, None, :]
    ).astype(jnp.int32)
    slot_rank = jnp.sum((jnp.cumsum(one_hot, 1) - one_hot) * one_hot, -1)
    slot_index = (
        slot_rank + (jnp.arange(block_count, dtype=jnp.int32) * capacity)[:, None]
    ).reshape(-1)
    outgoing = jnp.zeros((experts, block_count * capacity, width), jnp.bfloat16)
    outgoing = outgoing.at[flat_routes, slot_index].set(jnp.repeat(normed, top_count, axis=0))
    grouped = expert_apply(
        lax.all_gather(
            lax.all_to_all(outgoing, "ep", split_axis=0, concat_axis=0, tiled=True),
            "tp",
            axis=1,
            tiled=True,
        ),
        w_gate,
        w_up,
        w_down,
    )
    group_total = lax.psum_scatter(
        grouped.astype(jnp.bfloat16), "tp", scatter_dimension=1, tiled=True
    ).astype(jnp.float32)
    returned = lax.all_to_all(
        group_total.astype(jnp.bfloat16), "ep", split_axis=0, concat_axis=0, tiled=True
    ).astype(group_total.dtype)
    routed = returned[flat_routes, slot_index].reshape(-1, top_count, width)
    mixture = jnp.sum(weights[:, :, None] * routed, 1)
    return (residual + mixture).astype(jnp.bfloat16)


def solution(mesh):
    return jax.shard_map(
        body,
        mesh=mesh,
        in_specs=(
            P("ep", None),
            P("ep", "tp"),
            P("ep", "tp"),
            P("ep", "tp"),
            P("ep", "tp", None, None),
            P("ep", "tp", None, None),
            P("ep"),
            P("tp", None),
            P(),
            P("ep", None),
            P("ep", None, "tp"),
            P("ep", None, "tp"),
            P("ep", "tp", None),
        ),
        out_specs=P(("ep", "tp"), None),
        check_vma=False,
    )
```

```python
import functools

import jax
import jax.numpy as jnp
from jax import lax
from jax.experimental import pallas as pl
from jax.experimental.pallas import tpu as pltpu
from jax.sharding import PartitionSpec as P

LANES = 128
MESH = pl.DeviceIdType.MESH


def attend(queries, new_keys, new_values, key_cache, value_cache, cache_lengths):
    seq_count, kv_count, head_dim, length = key_cache.shape
    new_count = queries.shape[0] // seq_count
    group_size = queries.shape[1] // (kv_count * head_dim)
    row_count = new_count * group_size
    scale = head_dim ** (-0.5)
    query_block = queries.reshape(seq_count, new_count, kv_count, group_size, head_dim)
    query_block = query_block.transpose(0, 2, 1, 3, 4).reshape(
        seq_count, kv_count, row_count, head_dim
    )
    fresh_keys = new_keys.reshape(seq_count, new_count, kv_count, head_dim).transpose(0, 2, 1, 3)
    fresh_values = new_values.reshape(seq_count, new_count, kv_count, head_dim).transpose(
        0, 2, 1, 3
    )
    cache_scores = (
        jnp.einsum("skrd,skdl->skrl", query_block, key_cache, preferred_element_type=jnp.float32)
        * scale
    )
    in_cache = jnp.arange(length)[None, :] < cache_lengths[:, None]
    cache_scores = jnp.where(in_cache[:, None, None, :], cache_scores, -1e30)
    fresh_scores = (
        jnp.einsum("skrd,sknd->skrn", query_block, fresh_keys, preferred_element_type=jnp.float32)
        * scale
    )
    causal = (jnp.arange(row_count) // group_size)[:, None] >= jnp.arange(new_count)[None, :]
    fresh_scores = jnp.where(causal[None, None, :, :], fresh_scores, -1e30)
    row_max = jnp.maximum(
        jnp.max(cache_scores, -1, keepdims=True), jnp.max(fresh_scores, -1, keepdims=True)
    )
    cache_exp = jnp.exp(cache_scores - row_max)
    fresh_exp = jnp.exp(fresh_scores - row_max)
    denom_sum = jnp.sum(cache_exp, -1, keepdims=True) + jnp.sum(fresh_exp, -1, keepdims=True)
    cache_probs = (cache_exp / denom_sum).astype(jnp.bfloat16)
    fresh_probs = (fresh_exp / denom_sum).astype(jnp.bfloat16)
    head_mix = jnp.einsum(
        "skrl,skdl->skrd", cache_probs, value_cache, preferred_element_type=jnp.float32
    )
    head_mix = head_mix + jnp.einsum(
        "skrn,sknd->skrd", fresh_probs, fresh_values, preferred_element_type=jnp.float32
    )
    head_mix = head_mix.reshape(seq_count, kv_count, new_count, group_size, head_dim).transpose(
        0, 2, 1, 3, 4
    )
    return head_mix.reshape(seq_count * new_count, kv_count * group_size * head_dim).astype(
        jnp.bfloat16
    )


def expert_apply(received, w_gate, w_up, w_down):
    width = received.shape[-1]
    flat_rows = received.reshape(-1, width)
    gate_proj = jnp.dot(flat_rows, w_gate[0], preferred_element_type=jnp.float32)
    up_proj = jnp.dot(flat_rows, w_up[0], preferred_element_type=jnp.float32)
    activated = ((up_proj + 1.0) * gate_proj * jax.nn.sigmoid(1.702 * gate_proj)).astype(
        jnp.bfloat16
    )
    partial_out = jnp.dot(activated, w_down[0], preferred_element_type=jnp.float32)
    return partial_out.reshape(received.shape[0], received.shape[1], width)


def layer_kernel(
    ep_size,
    experts,
    part_ref,
    hidden_ref,
    router_ref,
    mask_ref,
    gate_hbm,
    up_hbm,
    down_hbm,
    out_ref,
    got,
    res,
    rows,
    mixed,
    core_in,
    b_in,
    a_in,
    z_in,
    w_gate,
    w_up,
    w_down,
    load_sem,
    first_send,
    first_recv,
    gather_send,
    gather_recv,
    core_send,
    core_recv,
    sum_send,
    sum_recv,
):
    tp_size, block_rows, width = part_ref.shape
    padded = rows.shape[2]
    base = width // LANES * LANES
    offset = width - base
    line = ep_size // 2
    lane_slots = 4 * line
    ep = lax.axis_index("ep")
    tp = lax.axis_index("tp")
    x = ep % 2
    z = ep // 2
    core = tp % 2
    y = tp // 2
    x_step = 1 - 2 * x
    y_step = 2 - 4 * y
    partner = (ep, tp + 1 - 2 * core)
    a_dev = (ep + (1 - core) * x_step, tp + core * y_step)
    b_dev = (ep + core * x_step, tp + (1 - core) * y_step)

    def z_dev(k):
        return (((z + k) % line) * 2 + x, tp)

    loads = [
        pltpu.make_async_copy(gate_hbm.at[0], w_gate.at[pl.ds(0, width)], load_sem.at[0]),
        pltpu.make_async_copy(up_hbm.at[0], w_up.at[pl.ds(0, width)], load_sem.at[1]),
        pltpu.make_async_copy(down_hbm.at[0], w_down, load_sem.at[2]),
    ]
    for load in loads:
        load.start()

    peers = [(ep, (tp + k) % tp_size) for k in range(1, tp_size)]
    peers += [(ep + x_step, tp)] + [z_dev(k) for k in range(1, line)]
    barrier = pltpu.get_barrier_semaphore()
    for peer in peers:
        pl.semaphore_signal(barrier, inc=1, device_id=peer, device_id_type=MESH)
    pl.semaphore_wait(barrier, len(peers))

    def send(src, dst, send_sem, recv_sem, index, device):
        copy = pltpu.make_async_remote_copy(
            src_ref=src,
            dst_ref=dst,
            send_sem=send_sem.at[index],
            recv_sem=recv_sem.at[index],
            device_id=device,
            device_id_type=MESH,
        )
        copy.start()
        return copy

    firsts = []
    for k in (2, 1, 3):
        target = (tp + k) % tp_size
        firsts.append(
            send(part_ref.at[target], got.at[k - 1], first_send, first_recv, k - 1, (ep, target))
        )
    w_gate[width:, :] = jnp.zeros((padded - width, w_gate.shape[1]), w_gate.dtype)
    w_up[width:, :] = jnp.zeros((padded - width, w_up.shape[1]), w_up.dtype)
    res[:, base:] = jnp.zeros((block_rows, padded - base), jnp.float32)
    own = part_ref[tp].astype(jnp.float32)
    for copy in firsts:
        copy.wait_recv()
    for k in range(tp_size - 1):
        own = own + got[k].astype(jnp.float32)
    own = own.astype(jnp.bfloat16).astype(jnp.float32) + hidden_ref[...].astype(jnp.float32)
    res[:, :width] = own
    scale = lax.rsqrt(jnp.sum(own * own, -1, keepdims=True) * (1.0 / width) + 1e-05)
    normed = (res[...] * scale).astype(jnp.bfloat16)
    logits = jnp.dot(normed, router_ref[...], preferred_element_type=jnp.float32)
    lane = lax.broadcasted_iota(jnp.int32, (block_rows, LANES), 1)
    picked_exp = jnp.where(mask_ref[...] > 0, jnp.exp(logits), 0.0)
    second = lane >= offset + experts
    denom = jnp.sum(jnp.where(second, 0.0, picked_exp), -1, keepdims=True)
    weights = picked_exp / denom
    high = weights.astype(jnp.bfloat16).astype(jnp.float32)
    tail = jnp.where(second, weights - high, high)
    tail = jnp.where(lane < offset, normed[:, base:].astype(jnp.float32), tail)
    rows[0, :, :base] = normed[:, :base]
    rows[0, :, base:] = tail.astype(jnp.bfloat16)

    moves = {}

    def spread(slot, device, source):
        moves[slot] = send(
            rows.at[source], rows.at[slot], gather_send, gather_recv, slot, device
        )

    def forward(slot):
        if slot < line:
            spread(line + slot, a_dev, slot)
        if slot < 2 * line:
            spread(2 * line + slot, b_dev, slot)
        spread(lane_slots + slot, partner, slot)

    near = [k for k in range(1, line) if k in (1, line - 1)]
    far = [k for k in range(1, line) if k not in near]
    order = near + far
    for k in order:
        spread(line - k, z_dev(k), 0)
    forward(0)
    for slot in [line - k for k in order] + list(range(line, 2 * line)):
        moves[slot].wait_recv()
        forward(slot)
    for load in loads:
        load.wait()
    share_lane = lax.broadcasted_iota(jnp.int32, (2 * line * block_rows, LANES), 1)
    chosen = (share_lane == offset + ep) | (share_lane == offset + experts + ep)

    def expert(start):
        count = 2 * line
        held = rows[start : start + count].reshape(count * block_rows, padded)
        gate = jnp.dot(held, w_gate[...], preferred_element_type=jnp.float32)
        up = jnp.dot(held, w_up[...], preferred_element_type=jnp.float32)
        active = ((up + 1.0) * gate * jax.nn.sigmoid(1.702 * gate)).astype(jnp.bfloat16)
        share = jnp.sum(
            jnp.where(chosen, held[:, base:].astype(jnp.float32), 0.0), -1, keepdims=True
        )
        step = 6 * LANES
        for low in range(0, width, step):
            size = min(step, width - low)
            out = jnp.dot(
                active, w_down[:, low : low + size], preferred_element_type=jnp.float32
            )
            mixed[start : start + count, :, low : low + size] = (
                (share * out).astype(jnp.bfloat16).reshape(count, block_rows, size)
            )

    half = 2 * line
    expert(0)
    for slot in range(half):
        moves[lane_slots + slot].wait_recv()
    expert(lane_slots)
    for slot in range(half, 2 * half):
        moves[slot].wait_recv()
        forward(slot)
    expert(half)
    for slot in range(half, 2 * half):
        moves[lane_slots + slot].wait_recv()
    expert(lane_slots + half)

    crossing = {}
    for quarter in (3, 2, 1, 0):
        crossing[quarter] = send(
            mixed.at[pl.ds(lane_slots + quarter * line, line)],
            core_in.at[pl.ds(quarter * line, line)],
            core_send,
            core_recv,
            quarter,
            partner,
        )

    sums = {}

    def reduce_send(slot, parts, dst, device):
        total = mixed[slot].astype(jnp.float32) + core_in[slot].astype(jnp.float32)
        for part in parts:
            total = total + part.astype(jnp.float32)
        mixed[slot] = total.astype(jnp.bfloat16)
        sums[slot] = send(mixed.at[slot], dst, sum_send, sum_recv, slot, device)

    for quarter in (3, 2):
        crossing[quarter].wait_recv()
        for slot in range(quarter * line, (quarter + 1) * line):
            reduce_send(slot, [], b_in.at[slot - half], b_dev)
    crossing[1].wait_recv()
    for slot in range(line, half):
        sums[half + slot].wait_recv()
        reduce_send(slot, [b_in[slot]], a_in.at[slot - line], a_dev)
    crossing[0].wait_recv()
    for slot in far + near:
        sums[half + slot].wait_recv()
        sums[line + slot].wait_recv()
        reduce_send(slot, [b_in[slot], a_in[slot]], z_in.at[slot - 1], z_dev(slot))
    sums[half].wait_recv()
    sums[line].wait_recv()
    total = res[:, :width] + mixed[0].astype(jnp.float32) + core_in[0].astype(jnp.float32)
    total = total + b_in[0].astype(jnp.float32) + a_in[0].astype(jnp.float32)
    for slot in far + near:
        sums[slot].wait_recv()
        total = total + z_in[slot - 1].astype(jnp.float32)
    out_ref[...] = total.astype(jnp.bfloat16)
    for copy in (
        firsts + list(moves.values()) + list(crossing.values()) + list(sums.values())
    ):
        copy.wait_send()


def fused_layer(partial_value, hidden, w_router, routes, w_gate, w_up, w_down):
    ep_size = lax.axis_size("ep")
    tp_size = lax.axis_size("tp")
    block_rows, width = hidden.shape
    experts = w_router.shape[1]
    hidden_share = w_gate.shape[2]
    base = width // LANES * LANES
    offset = width - base
    padded = base + LANES
    line = ep_size // 2
    slots = 8 * line
    room = LANES - offset - 2 * experts
    router = jnp.pad(
        jnp.concatenate([w_router, w_router], 1), ((0, padded - width), (offset, room))
    )
    named = jnp.any(routes[:, :, None] == jnp.arange(experts)[None, None, :], 1)
    named = named.astype(jnp.float32)
    mask = jnp.pad(jnp.concatenate([named, named], 1), ((0, 0), (offset, room)))
    vmem = pl.BlockSpec(memory_space=pltpu.VMEM)
    any_space = pl.BlockSpec(memory_space=pl.ANY)
    dma = pltpu.SemaphoreType.DMA
    bf16 = jnp.bfloat16
    return pl.pallas_call(
        functools.partial(layer_kernel, ep_size, experts),
        out_shape=jax.ShapeDtypeStruct((block_rows, width), bf16),
        in_specs=[vmem] * 4 + [any_space] * 3,
        out_specs=vmem,
        scratch_shapes=[
            pltpu.VMEM((tp_size - 1, block_rows, width), bf16),
            pltpu.VMEM((block_rows, padded), jnp.float32),
            pltpu.VMEM((slots, block_rows, padded), bf16),
            pltpu.VMEM((slots, block_rows, width), bf16),
            pltpu.VMEM((slots // 2, block_rows, width), bf16),
            pltpu.VMEM((slots // 4, block_rows, width), bf16),
            pltpu.VMEM((slots // 8, block_rows, width), bf16),
            pltpu.VMEM((line - 1, block_rows, width), bf16),
            pltpu.VMEM((padded, hidden_share), bf16),
            pltpu.VMEM((padded, hidden_share), bf16),
            pltpu.VMEM((hidden_share, width), bf16),
            dma((3,)),
            dma((tp_size - 1,)),
            dma((tp_size - 1,)),
            dma((slots,)),
            dma((slots,)),
            dma((4,)),
            dma((4,)),
            dma((slots // 2,)),
            dma((slots // 2,)),
        ],
        compiler_params=pltpu.CompilerParams(
            collective_id=0, has_side_effects=True, vmem_limit_bytes=48 * 1024 * 1024
        ),
    )(
        partial_value.reshape(tp_size, block_rows, width),
        hidden,
        router,
        mask,
        w_gate,
        w_up,
        w_down,
    )


def body(
    hidden,
    queries,
    new_keys,
    new_values,
    key_cache,
    value_cache,
    cache_lengths,
    w_out,
    w_router,
    routes,
    w_gate,
    w_up,
    w_down,
):
    tp_size = lax.axis_size("tp")
    tp_index = lax.axis_index("tp")
    width = hidden.shape[1]
    block_rows = hidden.shape[0] // tp_size
    top_count = routes.shape[1]
    experts = w_router.shape[1]
    capacity = min(block_rows, max(2, (2 * block_rows * top_count + experts - 1) // experts))
    start_row = tp_index * block_rows
    attended = attend(queries, new_keys, new_values, key_cache, value_cache, cache_lengths)
    partial_value = jnp.dot(attended, w_out, preferred_element_type=jnp.float32)
    fits = width % LANES + 2 * experts <= LANES and experts == lax.axis_size("ep")
    if capacity >= block_rows and tp_size == 4 and experts % 2 == 0 and experts > 2 and fits:
        return fused_layer(
            partial_value.astype(jnp.bfloat16),
            lax.dynamic_slice_in_dim(hidden, start_row, block_rows, 0),
            w_router,
            lax.dynamic_slice_in_dim(routes, start_row, block_rows, 0),
            w_gate,
            w_up,
            w_down,
        )
    summed = lax.psum_scatter(
        partial_value.astype(jnp.bfloat16), "tp", scatter_dimension=0, tiled=True
    ).astype(jnp.float32)
    residual = (
        lax.dynamic_slice_in_dim(hidden, start_row, block_rows, 0).astype(jnp.float32) + summed
    )
    local_routes = lax.dynamic_slice_in_dim(routes, start_row, block_rows, 0)
    block_count = 1
    normed = (
        residual * lax.rsqrt(jnp.mean(residual * residual, -1, keepdims=True) + 1e-05)
    ).astype(jnp.bfloat16)
    logits = jnp.dot(normed, w_router, preferred_element_type=jnp.float32)
    expert_ids = jnp.arange(experts, dtype=jnp.int32)
    matches = local_routes[:, :, None] == expert_ids[None, None, :]
    picked = jnp.sum(jnp.where(matches, logits[:, None, :], 0.0), -1)
    picked_exp = jnp.exp(picked)
    weights = picked_exp / jnp.sum(picked_exp, -1, keepdims=True)
    flat_routes = local_routes.reshape(-1)
    one_hot = (
        flat_routes.reshape(block_count, block_rows * top_count)[:, :, None]
        == expert_ids[None, None, :]
    ).astype(jnp.int32)
    slot_rank = jnp.sum((jnp.cumsum(one_hot, 1) - one_hot) * one_hot, -1)
    slot_index = (
        slot_rank + (jnp.arange(block_count, dtype=jnp.int32) * capacity)[:, None]
    ).reshape(-1)
    outgoing = jnp.zeros((experts, block_count * capacity, width), jnp.bfloat16)
    outgoing = outgoing.at[flat_routes, slot_index].set(jnp.repeat(normed, top_count, axis=0))
    grouped = expert_apply(
        lax.all_gather(
            lax.all_to_all(outgoing, "ep", split_axis=0, concat_axis=0, tiled=True),
            "tp",
            axis=1,
            tiled=True,
        ),
        w_gate,
        w_up,
        w_down,
    )
    group_total = lax.psum_scatter(
        grouped.astype(jnp.bfloat16), "tp", scatter_dimension=1, tiled=True
    ).astype(jnp.float32)
    returned = lax.all_to_all(
        group_total.astype(jnp.bfloat16), "ep", split_axis=0, concat_axis=0, tiled=True
    ).astype(group_total.dtype)
    routed = returned[flat_routes, slot_index].reshape(-1, top_count, width)
    mixture = jnp.sum(weights[:, :, None] * routed, 1)
    return (residual + mixture).astype(jnp.bfloat16)


def solution(mesh):
    return jax.shard_map(
        body,
        mesh=mesh,
        in_specs=(
            P("ep", None),
            P("ep", "tp"),
            P("ep", "tp"),
            P("ep", "tp"),
            P("ep", "tp", None, None),
            P("ep", "tp", None, None),
            P("ep"),
            P("tp", None),
            P(),
            P("ep", None),
            P("ep", None, "tp"),
            P("ep", None, "tp"),
            P("ep", "tp", None),
        ),
        out_specs=P(("ep", "tp"), None),
        check_vma=False,
    )
```

```python
import functools

import jax
import jax.numpy as jnp
from jax import lax
from jax.experimental import pallas as pl
from jax.experimental.pallas import tpu as pltpu
from jax.sharding import PartitionSpec as P

LANES = 128
MESH = pl.DeviceIdType.MESH


def attend(queries, new_keys, new_values, key_cache, value_cache, cache_lengths):
    seq_count, kv_count, head_dim, length = key_cache.shape
    new_count = queries.shape[0] // seq_count
    group_size = queries.shape[1] // (kv_count * head_dim)
    row_count = new_count * group_size
    scale = head_dim ** (-0.5)
    query_block = queries.reshape(seq_count, new_count, kv_count, group_size, head_dim)
    query_block = query_block.transpose(0, 2, 1, 3, 4).reshape(
        seq_count, kv_count, row_count, head_dim
    )
    fresh_keys = new_keys.reshape(seq_count, new_count, kv_count, head_dim).transpose(0, 2, 1, 3)
    fresh_values = new_values.reshape(seq_count, new_count, kv_count, head_dim).transpose(
        0, 2, 1, 3
    )
    cache_scores = (
        jnp.einsum("skrd,skdl->skrl", query_block, key_cache, preferred_element_type=jnp.float32)
        * scale
    )
    in_cache = jnp.arange(length)[None, :] < cache_lengths[:, None]
    cache_scores = jnp.where(in_cache[:, None, None, :], cache_scores, -1e30)
    fresh_scores = (
        jnp.einsum("skrd,sknd->skrn", query_block, fresh_keys, preferred_element_type=jnp.float32)
        * scale
    )
    causal = (jnp.arange(row_count) // group_size)[:, None] >= jnp.arange(new_count)[None, :]
    fresh_scores = jnp.where(causal[None, None, :, :], fresh_scores, -1e30)
    row_max = jnp.maximum(
        jnp.max(cache_scores, -1, keepdims=True), jnp.max(fresh_scores, -1, keepdims=True)
    )
    cache_exp = jnp.exp(cache_scores - row_max)
    fresh_exp = jnp.exp(fresh_scores - row_max)
    denom_sum = jnp.sum(cache_exp, -1, keepdims=True) + jnp.sum(fresh_exp, -1, keepdims=True)
    cache_probs = (cache_exp / denom_sum).astype(jnp.bfloat16)
    fresh_probs = (fresh_exp / denom_sum).astype(jnp.bfloat16)
    head_mix = jnp.einsum(
        "skrl,skdl->skrd", cache_probs, value_cache, preferred_element_type=jnp.float32
    )
    head_mix = head_mix + jnp.einsum(
        "skrn,sknd->skrd", fresh_probs, fresh_values, preferred_element_type=jnp.float32
    )
    head_mix = head_mix.reshape(seq_count, kv_count, new_count, group_size, head_dim).transpose(
        0, 2, 1, 3, 4
    )
    return head_mix.reshape(seq_count * new_count, kv_count * group_size * head_dim).astype(
        jnp.bfloat16
    )


def expert_apply(received, w_gate, w_up, w_down):
    width = received.shape[-1]
    flat_rows = received.reshape(-1, width)
    gate_proj = jnp.dot(flat_rows, w_gate[0], preferred_element_type=jnp.float32)
    up_proj = jnp.dot(flat_rows, w_up[0], preferred_element_type=jnp.float32)
    activated = ((up_proj + 1.0) * gate_proj * jax.nn.sigmoid(1.702 * gate_proj)).astype(
        jnp.bfloat16
    )
    partial_out = jnp.dot(activated, w_down[0], preferred_element_type=jnp.float32)
    return partial_out.reshape(received.shape[0], received.shape[1], width)


def layer_kernel(
    ep_size,
    experts,
    part_ref,
    hidden_ref,
    router_ref,
    routes_ref,
    gate_hbm,
    up_hbm,
    down_hbm,
    out_ref,
    got,
    res,
    rows,
    mixed,
    core_in,
    b_in,
    a_in,
    z_in,
    w_gate,
    w_up,
    w_down,
    router,
    load_sem,
    first_send,
    first_recv,
    gather_send,
    gather_recv,
    core_send,
    core_recv,
    sum_send,
    sum_recv,
):
    tp_size, block_rows, width = part_ref.shape
    padded = rows.shape[2]
    base = width // LANES * LANES
    offset = width - base
    line = ep_size // 2
    lane_slots = 4 * line
    ep = lax.axis_index("ep")
    tp = lax.axis_index("tp")
    x = ep % 2
    z = ep // 2
    core = tp % 2
    y = tp // 2
    x_step = 1 - 2 * x
    y_step = 2 - 4 * y
    partner = (ep, tp + 1 - 2 * core)
    a_dev = (ep + (1 - core) * x_step, tp + core * y_step)
    b_dev = (ep + core * x_step, tp + (1 - core) * y_step)

    def z_dev(k):
        return (((z + k) % line) * 2 + x, tp)

    loads = [
        pltpu.make_async_copy(gate_hbm.at[0], w_gate.at[pl.ds(0, width)], load_sem.at[0]),
        pltpu.make_async_copy(up_hbm.at[0], w_up.at[pl.ds(0, width)], load_sem.at[1]),
        pltpu.make_async_copy(down_hbm.at[0], w_down, load_sem.at[2]),
    ]
    for load in loads:
        load.start()

    peers = [(ep, (tp + k) % tp_size) for k in range(1, tp_size)]
    peers += [(ep + x_step, tp)] + [z_dev(k) for k in range(1, line)]
    barrier = pltpu.get_barrier_semaphore()
    for peer in peers:
        pl.semaphore_signal(barrier, inc=1, device_id=peer, device_id_type=MESH)
    pl.semaphore_wait(barrier, len(peers))

    def send(src, dst, send_sem, recv_sem, index, device):
        copy = pltpu.make_async_remote_copy(
            src_ref=src,
            dst_ref=dst,
            send_sem=send_sem.at[index],
            recv_sem=recv_sem.at[index],
            device_id=device,
            device_id_type=MESH,
        )
        copy.start()
        return copy

    firsts = []
    for k in (2, 1, 3):
        target = (tp + k) % tp_size
        firsts.append(
            send(part_ref.at[target], got.at[k - 1], first_send, first_recv, k - 1, (ep, target))
        )
    w_gate[width:, :] = jnp.zeros((padded - width, w_gate.shape[1]), w_gate.dtype)
    w_up[width:, :] = jnp.zeros((padded - width, w_up.shape[1]), w_up.dtype)
    router[...] = jnp.zeros(router.shape, router.dtype)
    router[offset : offset + experts, :width] = router_ref[...]
    router[offset + experts : offset + 2 * experts, :width] = router_ref[...]
    res[:, base:] = jnp.zeros((block_rows, padded - base), jnp.float32)
    own = part_ref[tp].astype(jnp.float32)
    for copy in firsts:
        copy.wait_recv()
    for k in range(tp_size - 1):
        own = own + got[k].astype(jnp.float32)
    mine = pl.ds(pl.multiple_of(tp * block_rows, block_rows), block_rows)
    own = own.astype(jnp.bfloat16).astype(jnp.float32) + hidden_ref[mine, :].astype(jnp.float32)
    res[:, :width] = own
    scale = lax.rsqrt(jnp.sum(own * own, -1, keepdims=True) * (1.0 / width) + 1e-05)
    normed = (res[...] * scale).astype(jnp.bfloat16)
    logits = lax.dot_general(
        normed, router[...], (((1,), (1,)), ((), ())), preferred_element_type=jnp.float32
    )
    lane = lax.broadcasted_iota(jnp.int32, (block_rows, LANES), 1)
    second = lane >= offset + experts
    lane_expert = jnp.where(second, lane - offset - experts, lane - offset)
    routes = routes_ref[mine, :]
    named = lane_expert == routes[:, 0:1]
    for r in range(1, routes.shape[1]):
        named = named | (lane_expert == routes[:, r : r + 1])
    picked_exp = jnp.where(named, jnp.exp(logits), 0.0)
    denom = jnp.sum(jnp.where(second, 0.0, picked_exp), -1, keepdims=True)
    weights = picked_exp / denom
    high = weights.astype(jnp.bfloat16).astype(jnp.float32)
    tail = jnp.where(second, weights - high, high)
    tail = jnp.where(lane < offset, normed[:, base:].astype(jnp.float32), tail)
    rows[0, :, :base] = normed[:, :base]
    rows[0, :, base:] = tail.astype(jnp.bfloat16)

    moves = {}

    def spread(slot, device, source):
        moves[slot] = send(
            rows.at[source], rows.at[slot], gather_send, gather_recv, slot, device
        )

    def forward(slot):
        if slot < line:
            spread(line + slot, a_dev, slot)
        if slot < 2 * line:
            spread(2 * line + slot, b_dev, slot)
        spread(lane_slots + slot, partner, slot)

    near = [k for k in range(1, line) if k in (1, line - 1)]
    far = [k for k in range(1, line) if k not in near]
    order = near + far
    for k in order:
        spread(line - k, z_dev(k), 0)
    forward(0)
    for slot in [line - k for k in order] + list(range(line, 2 * line)):
        moves[slot].wait_recv()
        forward(slot)
    for load in loads:
        load.wait()
    share_lane = lax.broadcasted_iota(jnp.int32, (2 * line * block_rows, LANES), 1)
    chosen = (share_lane == offset + ep) | (share_lane == offset + experts + ep)

    def expert(start):
        count = 2 * line
        held = rows[start : start + count].reshape(count * block_rows, padded)
        gate = jnp.dot(held, w_gate[...], preferred_element_type=jnp.float32)
        up = jnp.dot(held, w_up[...], preferred_element_type=jnp.float32)
        active = ((up + 1.0) * gate * jax.nn.sigmoid(1.702 * gate)).astype(jnp.bfloat16)
        share = jnp.sum(
            jnp.where(chosen, held[:, base:].astype(jnp.float32), 0.0), -1, keepdims=True
        )
        step = 6 * LANES
        for low in range(0, width, step):
            size = min(step, width - low)
            out = lax.dot_general(
                active,
                w_down[low : low + size, :],
                (((1,), (1,)), ((), ())),
                preferred_element_type=jnp.float32,
            )
            mixed[start : start + count, :, low : low + size] = (
                (share * out).astype(jnp.bfloat16).reshape(count, block_rows, size)
            )

    half = 2 * line
    crossing = {}
    sums = {}

    def cross(quarter):
        crossing[quarter] = send(
            mixed.at[pl.ds(lane_slots + quarter * line, line)],
            core_in.at[pl.ds(quarter * line, line)],
            core_send,
            core_recv,
            quarter,
            partner,
        )

    def reduce_send(slot, parts, dst, device):
        total = mixed[slot].astype(jnp.float32) + core_in[slot].astype(jnp.float32)
        for part in parts:
            total = total + part.astype(jnp.float32)
        mixed[slot] = total.astype(jnp.bfloat16)
        sums[slot] = send(mixed.at[slot], dst, sum_send, sum_recv, slot, device)

    expert(0)
    for slot in range(half):
        moves[lane_slots + slot].wait_recv()
    expert(lane_slots)
    cross(1)
    cross(0)
    for slot in range(half, 2 * half):
        moves[slot].wait_recv()
        forward(slot)
    crossing[1].wait_recv()
    for slot in range(line, half):
        reduce_send(slot, [], a_in.at[slot - line], a_dev)
    for slot in range(half, 2 * half):
        moves[lane_slots + slot].wait_recv()
    expert(lane_slots + half)
    cross(3)
    cross(2)
    expert(half)
    crossing[3].wait_recv()
    for slot in range(3 * line, 4 * line):
        reduce_send(slot, [], a_in.at[slot - half], a_dev)
    crossing[2].wait_recv()
    for slot in range(half, 3 * line):
        sums[line + slot].wait_recv()
        reduce_send(slot, [a_in[slot - line]], b_in.at[slot - half], b_dev)
    crossing[0].wait_recv()
    for slot in far + near:
        sums[line + slot].wait_recv()
        sums[half + slot].wait_recv()
        reduce_send(slot, [b_in[slot], a_in[slot]], z_in.at[slot - 1], z_dev(slot))
    sums[half].wait_recv()
    sums[line].wait_recv()
    total = res[:, :width] + mixed[0].astype(jnp.float32) + core_in[0].astype(jnp.float32)
    total = total + b_in[0].astype(jnp.float32) + a_in[0].astype(jnp.float32)
    for slot in far + near:
        sums[slot].wait_recv()
        total = total + z_in[slot - 1].astype(jnp.float32)
    out_ref[...] = total.astype(jnp.bfloat16)
    for copy in (
        firsts + list(moves.values()) + list(crossing.values()) + list(sums.values())
    ):
        copy.wait_send()


def fused_layer(partial_value, hidden, w_router, routes, w_gate, w_up, w_down):
    ep_size = lax.axis_size("ep")
    tp_size = lax.axis_size("tp")
    width = hidden.shape[1]
    block_rows = hidden.shape[0] // tp_size
    experts = w_router.shape[1]
    hidden_share = w_gate.shape[2]
    base = width // LANES * LANES
    padded = base + LANES
    line = ep_size // 2
    slots = 8 * line
    vmem = pl.BlockSpec(memory_space=pltpu.VMEM)
    any_space = pl.BlockSpec(memory_space=pl.ANY)
    dma = pltpu.SemaphoreType.DMA
    bf16 = jnp.bfloat16
    return pl.pallas_call(
        functools.partial(layer_kernel, ep_size, experts),
        out_shape=jax.ShapeDtypeStruct((block_rows, width), bf16),
        in_specs=[vmem] * 4 + [any_space] * 3,
        out_specs=vmem,
        scratch_shapes=[
            pltpu.VMEM((tp_size - 1, block_rows, width), bf16),
            pltpu.VMEM((block_rows, padded), jnp.float32),
            pltpu.VMEM((slots, block_rows, padded), bf16),
            pltpu.VMEM((slots, block_rows, width), bf16),
            pltpu.VMEM((slots // 2, block_rows, width), bf16),
            pltpu.VMEM((slots // 8, block_rows, width), bf16),
            pltpu.VMEM((slots // 4, block_rows, width), bf16),
            pltpu.VMEM((line - 1, block_rows, width), bf16),
            pltpu.VMEM((padded, hidden_share), bf16),
            pltpu.VMEM((padded, hidden_share), bf16),
            pltpu.VMEM((width, hidden_share), bf16),
            pltpu.VMEM((LANES, padded), bf16),
            dma((3,)),
            dma((tp_size - 1,)),
            dma((tp_size - 1,)),
            dma((slots,)),
            dma((slots,)),
            dma((4,)),
            dma((4,)),
            dma((slots // 2,)),
            dma((slots // 2,)),
        ],
        compiler_params=pltpu.CompilerParams(
            collective_id=0, has_side_effects=True, vmem_limit_bytes=67043328
        ),
    )(
        partial_value.reshape(tp_size, block_rows, width),
        hidden,
        w_router.T,
        routes,
        w_gate,
        w_up,
        jnp.swapaxes(w_down, 1, 2),
    )


def body(
    hidden,
    queries,
    new_keys,
    new_values,
    key_cache,
    value_cache,
    cache_lengths,
    w_out,
    w_router,
    routes,
    w_gate,
    w_up,
    w_down,
):
    tp_size = lax.axis_size("tp")
    tp_index = lax.axis_index("tp")
    width = hidden.shape[1]
    block_rows = hidden.shape[0] // tp_size
    top_count = routes.shape[1]
    experts = w_router.shape[1]
    capacity = min(block_rows, max(2, (2 * block_rows * top_count + experts - 1) // experts))
    start_row = tp_index * block_rows
    attended = attend(queries, new_keys, new_values, key_cache, value_cache, cache_lengths)
    partial_value = jnp.dot(attended, w_out, preferred_element_type=jnp.float32)
    fits = width % LANES + 2 * experts <= LANES and experts == lax.axis_size("ep")
    if capacity >= block_rows and tp_size == 4 and experts % 2 == 0 and experts > 2 and fits:
        return fused_layer(
            partial_value.astype(jnp.bfloat16),
            hidden,
            w_router,
            routes,
            w_gate,
            w_up,
            w_down,
        )
    summed = lax.psum_scatter(
        partial_value.astype(jnp.bfloat16), "tp", scatter_dimension=0, tiled=True
    ).astype(jnp.float32)
    residual = (
        lax.dynamic_slice_in_dim(hidden, start_row, block_rows, 0).astype(jnp.float32) + summed
    )
    local_routes = lax.dynamic_slice_in_dim(routes, start_row, block_rows, 0)
    block_count = 1
    normed = (
        residual * lax.rsqrt(jnp.mean(residual * residual, -1, keepdims=True) + 1e-05)
    ).astype(jnp.bfloat16)
    logits = jnp.dot(normed, w_router, preferred_element_type=jnp.float32)
    expert_ids = jnp.arange(experts, dtype=jnp.int32)
    matches = local_routes[:, :, None] == expert_ids[None, None, :]
    picked = jnp.sum(jnp.where(matches, logits[:, None, :], 0.0), -1)
    picked_exp = jnp.exp(picked)
    weights = picked_exp / jnp.sum(picked_exp, -1, keepdims=True)
    flat_routes = local_routes.reshape(-1)
    one_hot = (
        flat_routes.reshape(block_count, block_rows * top_count)[:, :, None]
        == expert_ids[None, None, :]
    ).astype(jnp.int32)
    slot_rank = jnp.sum((jnp.cumsum(one_hot, 1) - one_hot) * one_hot, -1)
    slot_index = (
        slot_rank + (jnp.arange(block_count, dtype=jnp.int32) * capacity)[:, None]
    ).reshape(-1)
    outgoing = jnp.zeros((experts, block_count * capacity, width), jnp.bfloat16)
    outgoing = outgoing.at[flat_routes, slot_index].set(jnp.repeat(normed, top_count, axis=0))
    grouped = expert_apply(
        lax.all_gather(
            lax.all_to_all(outgoing, "ep", split_axis=0, concat_axis=0, tiled=True),
            "tp",
            axis=1,
            tiled=True,
        ),
        w_gate,
        w_up,
        w_down,
    )
    group_total = lax.psum_scatter(
        grouped.astype(jnp.bfloat16), "tp", scatter_dimension=1, tiled=True
    ).astype(jnp.float32)
    returned = lax.all_to_all(
        group_total.astype(jnp.bfloat16), "ep", split_axis=0, concat_axis=0, tiled=True
    ).astype(group_total.dtype)
    routed = returned[flat_routes, slot_index].reshape(-1, top_count, width)
    mixture = jnp.sum(weights[:, :, None] * routed, 1)
    return (residual + mixture).astype(jnp.bfloat16)


def solution(mesh):
    return jax.shard_map(
        body,
        mesh=mesh,
        in_specs=(
            P("ep", None),
            P("ep", "tp"),
            P("ep", "tp"),
            P("ep", "tp"),
            P("ep", "tp", None, None),
            P("ep", "tp", None, None),
            P("ep"),
            P("tp", None),
            P(),
            P("ep", None),
            P("ep", None, "tp"),
            P("ep", None, "tp"),
            P("ep", "tp", None),
        ),
        out_specs=P(("ep", "tp"), None),
        check_vma=False,
    )
```
